32 devices in a mesh: gx: 4 (over y, x), gy: 8 (over z, core).
Axes of the slice: x: 2, y: 2, z: 4, core: 2. Of those that a mesh axis runs over, the one named last changes fastest.
Arguments:
- value_field: float32 [4, 24, 48, 1536], P(None, 'gx', 'gy'), may hold values from -16 to 17
- target_mask: int32 [4, 24, 48, 1536], P(None, 'gx', 'gy'), may hold values 0 or 1
- obstacle_mask: int32 [4, 24, 48, 1536], P(None, 'gx', 'gy'), may hold values 0 or 1
- drift_gains: float32 [5], replicated, may hold values from 0.5 to 2
- control_costs: float32 [5], replicated, may hold values from 0.25 to 1
Outputs:
- reach_value: float32 [4, 24, 48, 1536], P(None, 'gx', 'gy')
- time_steps: float32 [3], replicated
The draws below stay inside these ranges and needn't reach their ends.
All inputs are finite; a program needn't handle non-finite values. No bound on the sum of `target_mask` or of `obstacle_mask` on one device may be relied on, other than what follows from the above.
Results may differ from the reference program's by a relative error of at most 0.0003.
Values sent between devices are 32-bit elements; how exact they have to be, the bound alone decides.
No kernel may reach another device: no remote copies, remote signals or barrier semaphores. Data moves between devices by JAX's collectives and lax.ppermute only.
A program may use at most 128 MiB of HBM per device.

```python
import math
import jax
import jax.numpy as jnp
from jax import lax

PLANES = 4
N3 = 32
N4 = 48
GRID = 96
STEPS = 3
NA = 24
NB = 48


def draw_value_field(key, part):
    base_key = jax.random.fold_in(key, 11)
    rough_key, row_key, col_key = jax.random.split(base_key, 3)
    grid_shape = (PLANES, NA, NB, N3 * N4)
    rough_part = jnp.clip(jax.random.normal(rough_key, grid_shape, jnp.float32), -4.0, 4.0)
    row_scale = jnp.exp(jax.random.uniform(row_key, (NA,), jnp.float32, -math.log(2.0), math.log(2.0)))
    col_scale = jnp.exp(jax.random.uniform(col_key, (NB,), jnp.float32, -math.log(2.0), math.log(2.0)))
    return rough_part * row_scale[None, :, None, None] * col_scale[None, None, :, None]


def with_ends(values, own_key, smallest, largest):
    place = [jax.random.randint(jax.random.fold_in(own_key, axis), (), 0, length) for axis, length in enumerate(values.shape)]
    main_axis = values.shape.index(max(values.shape))
    neighbour = place[:main_axis] + [(place[main_axis] + 1) % values.shape[main_axis]] + place[main_axis + 1:]
    return values.at[tuple(place)].set(smallest).at[tuple(neighbour)].set(largest)


def setup_inputs(seed: int = 0) -> dict:
    splits = jax.random.split(jax.random.key(seed), 6)
    return {
        "value_field": draw_value_field(jax.random.fold_in(splits[5], 71), 0),
        "target_mask": with_ends((jax.random.randint(splits[1], (PLANES, NA, NB, N3 * N4), 0, 4) < 1).astype(jnp.int32), jax.random.fold_in(splits[1], 1), 0, 1),
        "obstacle_mask": with_ends((jax.random.randint(splits[2], (PLANES, NA, NB, N3 * N4), 0, 5) < 1).astype(jnp.int32), jax.random.fold_in(splits[2], 1), 0, 1),
        "drift_gains": jnp.clip(jnp.exp(jax.random.uniform(splits[3], (5,), jnp.float32, math.log(0.5), math.log(2.0))), 0.5, 2.0),
        "control_costs": jnp.clip(jnp.exp(jax.random.uniform(splits[4], (5,), jnp.float32, math.log(0.25), math.log(1.0))), 0.25, 1.0),
    }


courant = 0.5
weno_eps = 1e-6


def weno_side(diff_one, diff_two, diff_three, diff_four, diff_five):
    stencil_one = diff_one / 3.0 - 7.0 * diff_two / 6.0 + 11.0 * diff_three / 6.0
    stencil_two = -diff_two / 6.0 + 5.0 * diff_three / 6.0 + diff_four / 3.0
    stencil_three = diff_three / 3.0 + 5.0 * diff_four / 6.0 - diff_five / 6.0
    smooth_one = 13.0 / 12.0 * (diff_one - 2.0 * diff_two + diff_three) ** 2 + 0.25 * (diff_one - 4.0 * diff_two + 3.0 * diff_three) ** 2
    smooth_two = 13.0 / 12.0 * (diff_two - 2.0 * diff_three + diff_four) ** 2 + 0.25 * (diff_two - diff_four) ** 2
    smooth_three = 13.0 / 12.0 * (diff_three - 2.0 * diff_four + diff_five) ** 2 + 0.25 * (3.0 * diff_three - 4.0 * diff_four + diff_five) ** 2
    weight_one = 0.1 / (weno_eps + smooth_one) ** 2
    weight_two = 0.6 / (weno_eps + smooth_two) ** 2
    weight_three = 0.3 / (weno_eps + smooth_three) ** 2
    return (weight_one * stencil_one + weight_two * stencil_two + weight_three * stencil_three) / (weight_one + weight_two + weight_three)


def axis_slopes(shifted, spacing):
    differences = [shifted[offset + 1] - shifted[offset] for offset in range(6)]
    minus_slope = weno_side(differences[0], differences[1], differences[2], differences[3], differences[4]) / spacing
    plus_slope = weno_side(differences[5], differences[4], differences[3], differences[2], differences[1]) / spacing
    return minus_slope, plus_slope


def merged_shifts(interior, stride, position, extent):
    upward = []
    current = interior
    for offset in range(1, 4):
        current = jnp.where(position + offset <= extent - 1, jnp.roll(interior, -offset * stride, axis=-1), current)
        upward.append(current)
    downward = []
    current = interior
    for offset in range(1, 4):
        current = jnp.where(position - offset >= 0, jnp.roll(interior, offset * stride, axis=-1), current)
        downward.append(current)
    return [downward[2], downward[1], downward[0], interior, upward[0], upward[1], upward[2]]


def drift_field(first_pos, heading_one, heading_two, third_pos, fourth_pos, drift_gains):
    return [drift_gains[0] * (jnp.cos(heading_one) - 0.5 * jnp.cos(heading_two) + third_pos),
            drift_gains[1] * (fourth_pos - 0.3 * first_pos),
            drift_gains[2] * (third_pos + 0.5 * jnp.sin(heading_one)),
            drift_gains[3] * (jnp.sin(heading_two) - first_pos),
            drift_gains[4] * (jnp.cos(heading_one) * jnp.sin(heading_two) - fourth_pos)]


def local_bounds(drift_terms, slopes, control_costs, spacing_list):
    peaks = []
    for axis_number in range(5):
        scale = control_costs[axis_number] * spacing_list[axis_number]
        minus_peak = jnp.max(jnp.abs(drift_terms[axis_number] - scale * slopes[axis_number][0]))
        plus_peak = jnp.max(jnp.abs(drift_terms[axis_number] - scale * slopes[axis_number][1]))
        peaks.append(jnp.maximum(minus_peak, plus_peak))
    return jnp.stack(peaks)


def advance(interior, slopes, drift_terms, bounds, time_step, control_costs, spacing_list, target_plane, obstacle_plane):
    hamiltonian = jnp.zeros_like(interior)
    for axis_number in range(5):
        minus_slope, plus_slope = slopes[axis_number]
        middle = 0.5 * (minus_slope + plus_slope)
        hamiltonian = hamiltonian + drift_terms[axis_number] * middle - 0.5 * control_costs[axis_number] * spacing_list[axis_number] * middle * middle
        hamiltonian = hamiltonian - bounds[axis_number] * 0.5 * (plus_slope - minus_slope)
    advanced = interior - time_step * hamiltonian
    advanced = jnp.where(target_plane == 1, jnp.minimum(advanced, -0.5), advanced)
    return jnp.where(obstacle_plane == 1, jnp.maximum(advanced, 0.5), advanced)


def plane_state(padded, plane_index, drift_gains, spacing_list):
    center = lax.dynamic_index_in_dim(padded, plane_index, 0, keepdims=False)
    interior = center[3:-3, 3:-3]
    neighbours = [lax.dynamic_index_in_dim(padded, jnp.clip(plane_index + offset - 3, 0, PLANES - 1).astype(jnp.int32), 0, keepdims=False)[3:-3, 3:-3] for offset in range(7)]
    row_shifts = [center[offset:offset + NA, 3:-3] for offset in range(7)]
    col_shifts = [center[3:-3, offset:offset + NB] for offset in range(7)]
    lane_index = jnp.arange(N3 * N4, dtype=jnp.int32)
    slopes = [axis_slopes(neighbours, spacing_list[0]),
              axis_slopes(row_shifts, spacing_list[1]),
              axis_slopes(col_shifts, spacing_list[2]),
              axis_slopes(merged_shifts(interior, N4, lane_index // N4, N3), spacing_list[3]),
              axis_slopes(merged_shifts(interior, 1, lane_index % N4, N4), spacing_list[4])]
    first_pos = (plane_index.astype(jnp.float32) - PLANES / 2 + 0.5) * (2.0 / GRID)
    heading_one = ((2.0 * math.pi / NA) * jnp.arange(NA, dtype=jnp.float32)).reshape(NA, 1, 1)
    heading_two = ((2.0 * math.pi / NB) * jnp.arange(NB, dtype=jnp.float32)).reshape(1, NB, 1)
    third_pos = (((lane_index // N4).astype(jnp.float32) - N3 / 2 + 0.5) * (2.0 / GRID)).reshape(1, 1, -1)
    fourth_pos = (((lane_index % N4).astype(jnp.float32) - N4 / 2 + 0.5) * (2.0 / GRID)).reshape(1, 1, -1)
    drift_terms = drift_field(first_pos, heading_one, heading_two, third_pos, fourth_pos, drift_gains)
    return interior, slopes, drift_terms


def reference(value_field, target_mask, obstacle_mask, drift_gains, control_costs):
    spacing_list = [2.0 / GRID, 2.0 * math.pi / NA, 2.0 * math.pi / NB, 2.0 / GRID, 2.0 / GRID]
    spacing_array = jnp.array(spacing_list, dtype=jnp.float32)
    plane_ids = jnp.arange(PLANES, dtype=jnp.int32)
    value_now = value_field
    step_sizes = []
    for section_number in range(STEPS):
        padded = jnp.pad(value_now, ((0, 0), (3, 3), (3, 3), (0, 0)), mode="wrap")

        def bound_plane(plane_index):
            interior, slopes, drift_terms = plane_state(padded, plane_index, drift_gains, spacing_list)
            return local_bounds(drift_terms, slopes, control_costs, spacing_list)

        bounds = jnp.max(lax.map(bound_plane, plane_ids), axis=0)
        time_step = courant / (jnp.sum(bounds / spacing_array) + 1e-6)

        def move_plane(items):
            plane_index, target_plane, obstacle_plane = items
            interior, slopes, drift_terms = plane_state(padded, plane_index, drift_gains, spacing_list)
            return advance(interior, slopes, drift_terms, bounds, time_step, control_costs, spacing_list, target_plane, obstacle_plane)

        value_now = lax.map(move_plane, (plane_ids, target_mask, obstacle_mask))
        step_sizes.append(time_step)
    return value_now, jnp.stack(step_sizes)
```

```python
import math

import jax
import jax.numpy as jnp
import numpy as np
from jax import lax
from jax.experimental import pallas as pl
from jax.experimental.pallas import tpu as pltpu
from jax.sharding import PartitionSpec as P

N3 = 32
N4 = 48
GRID = 96
STEPS = 3


courant = 0.5
weno_eps = 1e-06
LANES = 128
QUARTERS = 4
HALO = 3
BIG = 3.0e38


def sub(a, b):
    if b is None:
        return a
    return -b if a is None else a - b


def mul(a, scalar):
    return None if a is None else a * scalar


def square_term(inner, outer):
    constant = 0.3 * weno_eps
    if inner is None and outer is None:
        return constant
    if outer is None:
        return inner * inner + constant
    scaled = outer * 0.55
    rest = scaled * scaled * (0.0975 / 0.3025) + constant
    lean = sub(inner, scaled)
    return lean * lean + rest


def middle_term(left, right):
    constant = 0.75 * weno_eps
    if left is None and right is None:
        return constant
    if left is None or right is None:
        own = right if left is None else left
        return own * own + constant
    slope = right - left
    return slope * slope + (left * 0.75 * right + constant)


def bend(e_left, e_mid, e_right):
    return sub(sub(e_right, e_mid), sub(e_mid, e_left)) if e_mid is not None else (
        e_left if e_right is None else (e_right if e_left is None else e_left + e_right)
    )


def interface(e_one, e_two, e_three, e_four, inverse, minus, plus):
    first = square_term(e_two, e_one)
    second = middle_term(e_two, e_three)
    third = square_term(e_three, e_four)
    weight_one = second * third
    weight_two = first * third
    weight_three = first * second
    weight_one = weight_one * weight_one
    weight_two = weight_two * weight_two * 37.5
    weight_three = weight_three * weight_three
    bend_low = bend(e_one, e_two, e_three)
    bend_high = bend(e_two, e_three, e_four)
    result = []
    common = weight_one + weight_two + weight_three
    if minus:
        top = weight_one * (bend_low * (inverse / 6.0)) if bend_low is not None else 0.0
        high = bend_high * (inverse / 12.0)
        lower = common + (weight_three + weight_three)
        result.append((top + weight_three * high * 3.0) / lower - high * 0.5)
    if plus:
        top = weight_three * (bend_high * (inverse / 6.0)) if bend_high is not None else 0.0
        low = bend_low * (inverse / 12.0)
        lower = common + (weight_one + weight_one)
        result.append((top + weight_one * low * 3.0) / lower - low * 0.5)
    return result


def central(d_before, d_after, e_before, e_after, inverse):
    total = d_after if d_before is None else (d_before if d_after is None else d_before + d_after)
    tilt = sub(e_after, e_before)
    return total * (0.5 * inverse) - tilt * (inverse / 12.0)


def line_slopes(differences, inverse, cells):
    bends = [
        None if differences[j] is None and differences[j + 1] is None
        else sub(differences[j + 1], differences[j])
        for j in range(len(differences) - 1)
    ]
    minus = []
    plus = []
    for face in range(cells + 1):
        window = bends[face : face + 4]
        values = interface(*window, inverse, face < cells, face > 0)
        if face < cells:
            minus.append(values[0])
        if face > 0:
            plus.append(values[-1])
    out = []
    for cell in range(cells):
        base = central(
            differences[cell + 2], differences[cell + 3], bends[cell + 1], bends[cell + 3], inverse
        )
        out.append((base + (plus[cell] - minus[cell]), plus[cell] + minus[cell]))
    return out


def flux(middle, jump, drift, kappa):
    tilt = drift - kappa * middle
    return middle * (drift + tilt), jnp.abs(tilt) + kappa * jnp.abs(jump)


def sublane_turn(value):
    return pltpu.roll(value, 4, 0)


def spacings(sizes):
    return [
        2.0 / GRID,
        2.0 * math.pi / sizes["row_total"],
        2.0 * math.pi / sizes["col_total"],
        2.0 / GRID,
        2.0 / GRID,
    ]


def lane_shift(tiles, count, turn):
    number = len(tiles)
    lane = lax.broadcasted_iota(jnp.int32, (8, LANES), 1)
    spun = [pltpu.roll(tile, (-count) % LANES, 1) for tile in tiles]
    out = []
    for index in range(number):
        if count > 0:
            other = index + 1
            inside = lane < LANES - count
        else:
            other = index - 1
            inside = lane >= -count
        if 0 <= other < number:
            out.append(jnp.where(inside, spun[index], spun[other]))
        elif turn:
            wrapped = pltpu.roll(spun[other % number], 7 if count > 0 else 1, 0)
            out.append(jnp.where(inside, spun[index], wrapped))
        else:
            out.append(spun[index])
    return out


def lane_axis(tiles, stride, inverse, position, extent, turn, gather):
    number = range(len(tiles))
    first = [position[t] == 0 for t in number]
    last = [position[t] == extent - 1 for t in number]
    near_last = [position[t] >= extent - 2 for t in number]
    ahead = lane_shift(tiles, stride, turn)
    steps = [jnp.where(last[t], 0.0, ahead[t] - tiles[t]) for t in number]
    before = lane_shift(steps, -stride, turn)
    if not turn:
        before = [jnp.where(first[0], 0.0, before[0])] + before[1:]
    bends = [steps[t] - before[t] for t in number]
    down = lane_shift(bends, -stride, turn)
    down = [jnp.where(first[t], 0.0, down[t]) for t in number]
    up = lane_shift(bends, stride, turn)
    up = [jnp.where(last[t], 0.0, up[t]) for t in number]
    far = lane_shift(bends, 2 * stride, turn)
    far = [jnp.where(near_last[t], 0.0, far[t]) for t in number]
    minus = []
    plus = []
    for t in number:
        low, high = interface(down[t], bends[t], up[t], far[t], inverse, True, True)
        minus.append(low)
        plus.append(high)
    minus = lane_shift(minus, -stride, turn)
    if gather:
        own = bends[-1]
        over = up[-1]
        for t in number[:-1]:
            own = jnp.where(first[t], bends[t], own)
            over = jnp.where(first[t], up[t], over)
        edge = interface(None, None, own, over, inverse, True, False)[0]
        minus = [jnp.where(first[t], edge, minus[t]) for t in number]
    else:
        edge = interface(None, None, bends[0], up[0], inverse, True, False)[0]
        minus = [jnp.where(first[0], edge, minus[0])] + minus[1:]
    out = []
    for t in number:
        base = central(before[t], steps[t], down[t], up[t], inverse)
        out.append((base + (plus[t] - minus[t]), plus[t] + minus[t]))
    return out


def angle_tables(sizes):
    a = np.arange(sizes["row_total"], dtype=np.float64) * (2.0 * math.pi / sizes["row_total"])
    b = np.arange(sizes["col_total"], dtype=np.float64) * (2.0 * math.pi / sizes["col_total"])
    return (
        np.stack([np.cos(a), np.sin(a)]).astype(np.float32),
        np.stack([np.cos(b), np.sin(b)]).astype(np.float32),
    )


def lane_tables(sizes):
    lane = np.arange(sizes["width"])
    quarter = np.arange(8) % QUARTERS
    third = quarter[:, None] * (sizes["width"] // N4) + lane[None, :] // N4
    fourth = np.broadcast_to(lane[None, :] % N4, third.shape)
    return np.stack([third, fourth]).astype(np.float32)


def plane_position(plane, planes):
    return float((plane - planes / 2 + 0.5) * (2.0 / GRID))


def position_of(index, extent):
    return (index - extent / 2 + 0.5) * (2.0 / GRID)


def column_vector(table, kind, base, group, half, width=LANES):
    sublane = lax.broadcasted_iota(jnp.int32, (8, width), 0)
    low = jnp.full((8, width), table[kind, base + group], jnp.float32)
    high = jnp.full((8, width), table[kind, base + group + half], jnp.float32)
    return jnp.where(sublane < QUARTERS, low, high)


def local_kernel(sizes, where_ref, gains, costs, rows_ref, cols_ref, lanes_ref, value, flow, jump, peak):
    planes, rows, groups, tiles = sizes["planes"], sizes["rows"], sizes["groups"], sizes["tiles"]
    spacing = spacings(sizes)
    inverse = [1.0 / h for h in spacing]
    kappa = [costs[i] * spacing[i] for i in range(5)]
    row_base = where_ref[0] * rows
    col_base = where_ref[1] * 2 * groups

    def body(step, peaks):
        row = step // groups
        group = step % groups
        cos_a = rows_ref[0, row_base + row]
        cos_b = column_vector(cols_ref, 0, col_base, group, groups)
        sin_b = column_vector(cols_ref, 1, col_base, group, groups)
        third = [lanes_ref[0, :, pl.ds(t * LANES, LANES)] for t in range(tiles)]
        fourth = [lanes_ref[1, :, pl.ds(t * LANES, LANES)] for t in range(tiles)]
        block = [
            [value[row, group, p, :, pl.ds(t * LANES, LANES)] for t in range(tiles)]
            for p in range(planes)
        ]
        peak_zero, peak_three, peak_four = peaks
        total = [[None] * tiles for _ in range(planes)]
        for t in range(tiles):
            steps = [block[p + 1][t] - block[p][t] for p in range(planes - 1)]
            slopes = line_slopes([None] * 3 + steps + [None] * 3, inverse[0], planes)
            drift = gains[0] * (cos_a - 0.5 * cos_b + position_of(third[t], N3))
            for p in range(planes):
                middle, half_jump = slopes[p]
                part, speed = flux(middle, half_jump, drift, kappa[0])
                peak_zero = jnp.maximum(peak_zero, speed)
                total[p][t] = part
                jump[0, row, group, p, :, pl.ds(t * LANES, LANES)] = half_jump
        for p in range(planes):
            slopes = lane_axis(block[p], N4, inverse[3], third, N3, True, False)
            drift = gains[3] * (sin_b - plane_position(p, planes))
            for t in range(tiles):
                middle, half_jump = slopes[t]
                part, speed = flux(middle, half_jump, drift, kappa[3])
                peak_three = jnp.maximum(peak_three, speed)
                total[p][t] = total[p][t] + part
                jump[1, row, group, p, :, pl.ds(t * LANES, LANES)] = half_jump
            slopes = lane_axis(block[p], 1, inverse[4], fourth, N4, False, True)
            for t in range(tiles):
                middle, half_jump = slopes[t]
                drift = gains[4] * (cos_a * sin_b - position_of(fourth[t], N4))
                part, speed = flux(middle, half_jump, drift, kappa[4])
                peak_four = jnp.maximum(peak_four, speed)
                jump[2, row, group, p, :, pl.ds(t * LANES, LANES)] = half_jump
                flow[row, group, p, :, pl.ds(t * LANES, LANES)] = total[p][t] + part
        return peak_zero, peak_three, peak_four

    zero = jnp.zeros((8, LANES), jnp.float32)
    peaks = lax.fori_loop(0, rows * groups, body, (zero, zero, zero))
    for i in range(3):
        peak[i] = peaks[i]


def column_kernel(sizes, where_ref, gains, costs, rows_ref, lanes_ref, value, left, right, flow, jump, peak):
    planes, rows, groups, tiles = sizes["planes"], sizes["rows"], sizes["groups"], sizes["tiles"]
    spacing = spacings(sizes)[2]
    kappa = costs[2] * spacing
    row_base = where_ref[0] * rows
    lower = lax.broadcasted_iota(jnp.int32, (8, LANES), 0) < QUARTERS

    def body(step, top):
        row = step // tiles
        lanes = pl.ds(pl.multiple_of((step % tiles) * LANES, LANES), LANES)
        third = lanes_ref[0, :, lanes]
        drift = gains[2] * (position_of(third, N3) + 0.5 * rows_ref[1, row_base + row])
        for p in range(planes):
            own = [value[row, g, p, :, lanes] for g in range(groups)]
            turned = [sublane_turn(own[g]) for g in range(groups)]
            packed_left = [left[row, k, p % (planes // 2), :, lanes] for k in range(HALO)]
            packed_right = [right[row, k, p % (planes // 2), :, lanes] for k in range(HALO)]
            if p >= planes // 2:
                packed_left = [sublane_turn(x) for x in packed_left]
            else:
                packed_right = [sublane_turn(x) for x in packed_right]
            below = [jnp.where(lower, packed_left[k], turned[groups - HALO + k]) for k in range(HALO)]
            above = [jnp.where(lower, turned[k], packed_right[k]) for k in range(HALO)]
            line = below + own + above
            steps = [line[j + 1] - line[j] for j in range(len(line) - 1)]
            slopes = line_slopes(steps, 1.0 / spacing, groups)
            for g in range(groups):
                middle, half_jump = slopes[g]
                part, speed = flux(middle, half_jump, drift, kappa)
                top = jnp.maximum(top, speed)
                flow[row, g, p, :, lanes] = part
                jump[row, g, p, :, lanes] = half_jump
        return top

    peak[0] = lax.fori_loop(0, rows * tiles, body, jnp.zeros((8, LANES), jnp.float32))


def row_kernel(sizes, gains, costs, lanes_ref, value, before, after, peak_local, peak_col, flow, jump, spread):
    planes, rows, groups, tiles = sizes["planes"], sizes["rows"], sizes["groups"], sizes["tiles"]
    spacing = spacings(sizes)[1]
    kappa = costs[1] * spacing

    def body(step, top):
        group = step // tiles
        lanes = pl.ds(pl.multiple_of((step % tiles) * LANES, LANES), LANES)
        fourth = position_of(lanes_ref[1, :, lanes], N4)
        for p in range(planes):
            line = [before[k, group, p, :, lanes] for k in range(HALO)]
            line += [value[r, group, p, :, lanes] for r in range(rows)]
            line += [after[k, group, p, :, lanes] for k in range(HALO)]
            steps = [line[j + 1] - line[j] for j in range(len(line) - 1)]
            slopes = line_slopes(steps, 1.0 / spacing, rows)
            drift = gains[1] * (fourth - 0.3 * plane_position(p, planes))
            for r in range(rows):
                middle, half_jump = slopes[r]
                part, speed = flux(middle, half_jump, drift, kappa)
                top = jnp.maximum(top, speed)
                flow[r, group, p, :, lanes] = part
                jump[r, group, p, :, lanes] = half_jump
        return top

    top = lax.fori_loop(0, groups * tiles, body, jnp.zeros((8, LANES), jnp.float32))
    found = [peak_local[0], top, peak_col[0], peak_local[1], peak_local[2]]
    sublane = lax.broadcasted_iota(jnp.int32, (8, LANES), 0)
    packed = jnp.zeros((8, LANES), jnp.float32)
    for i in range(5):
        widest = jnp.max(found[i], axis=0, keepdims=True)
        packed = jnp.where(sublane == i, widest, packed)
    for device in range(spread.shape[0]):
        spread[device] = packed


def update_kernel(sizes, value, ceiling, floor, flow_local, flow_col, flow_row, jump_local, jump_col, jump_row,
                  gathered, result, *rest):
    planes, rows, groups, tiles = sizes["planes"], sizes["rows"], sizes["groups"], sizes["tiles"]
    spacing = spacings(sizes)
    step_ref = rest[-1]
    best = gathered[0]
    for device in range(1, gathered.shape[0]):
        best = jnp.maximum(best, gathered[device])
    widest = jnp.max(best, axis=1, keepdims=True)
    bounds = [widest[i : i + 1, :] for i in range(5)]
    total = bounds[0] / spacing[0]
    for i in range(1, 5):
        total = total + bounds[i] / spacing[i]
    time_step = courant / (total + 1e-06)
    step_ref[...] = jnp.broadcast_to(time_step, (8, LANES))
    half_step = jnp.broadcast_to(time_step * 0.5, (8, LANES))
    weights = [jnp.broadcast_to(time_step * bounds[i], (8, LANES)) for i in range(5)]
    lower = lax.broadcasted_iota(jnp.int32, (8, LANES), 0) < QUARTERS

    def body(step, carry):
        row = step // groups
        group = step % groups
        for t in range(tiles):
            lanes = pl.ds(t * LANES, LANES)
            fresh = []
            for p in range(planes):
                at = (row, group, p, slice(None), lanes)
                flow = flow_local[at] + flow_col[at] + flow_row[at]
                moved = (
                    (weights[0] * jump_local[(0,) + at] + weights[3] * jump_local[(1,) + at])
                    + (weights[4] * jump_local[(2,) + at] + weights[2] * jump_col[at])
                ) + (weights[1] * jump_row[at] - half_step * flow)
                new = value[at] + moved
                new = jnp.maximum(jnp.minimum(new, ceiling[at]), floor[at])
                result[at] = new
                fresh.append(new)
        return carry

    lax.fori_loop(0, rows * groups, body, 0)
    if len(rest) > 1:
        send_pieces(sizes, result, *rest[:-1])


def send_pieces(sizes, value, first_rows, last_rows, first_cols, last_cols):
    planes, rows, groups, tiles = sizes["planes"], sizes["rows"], sizes["groups"], sizes["tiles"]
    lower = lax.broadcasted_iota(jnp.int32, (8, LANES), 0) < QUARTERS
    half = planes // 2
    for k in range(HALO):
        first_rows[k] = value[k]
        last_rows[k] = value[rows - HALO + k]

    def body(row, carry):
        for k in range(HALO):
            for p in range(half):
                for t in range(tiles):
                    lanes = pl.ds(t * LANES, LANES)
                    one = value[row, k, p, :, lanes]
                    two = value[row, k, p + half, :, lanes]
                    first_cols[row, k, p, :, lanes] = jnp.where(lower, one, sublane_turn(two))
                    one = value[row, groups - HALO + k, p, :, lanes]
                    two = value[row, groups - HALO + k, p + half, :, lanes]
                    last_cols[row, k, p, :, lanes] = jnp.where(lower, sublane_turn(one), two)
        return carry

    lax.fori_loop(0, rows, body, 0)


def prepare_kernel(sizes, value, *pieces):
    send_pieces(sizes, value, *pieces)


VMEM = pl.BlockSpec(memory_space=pltpu.VMEM)
SMEM = pl.BlockSpec(memory_space=pltpu.SMEM)


def call(kernel, sizes, outs, specs, name, flops):
    return pl.pallas_call(
        lambda *refs: kernel(sizes, *refs),
        out_shape=[jax.ShapeDtypeStruct(shape, jnp.float32) for shape in outs],
        in_specs=specs,
        out_specs=[VMEM] * len(outs),
        name=name,
        compiler_params=pltpu.CompilerParams(vmem_limit_bytes=48 * 1024 * 1024),
        cost_estimate=pl.CostEstimate(flops=flops, bytes_accessed=1000000, transcendentals=0),
    )


def to_blocks(array, sizes):
    planes, rows, groups = sizes["planes"], sizes["rows"], sizes["groups"]
    split = array.reshape(planes, rows, 2, groups, QUARTERS, sizes["width"])
    return split.transpose(1, 3, 0, 2, 4, 5).reshape(rows, groups, planes, 8, sizes["width"])


def from_blocks(blocks, sizes):
    planes, rows, groups = sizes["planes"], sizes["rows"], sizes["groups"]
    split = blocks.reshape(rows, groups, planes, 2, QUARTERS, sizes["width"])
    return split.transpose(2, 0, 3, 1, 4, 5).reshape(planes, rows, 2 * groups, QUARTERS * sizes["width"])


def body(value_field, target_mask, obstacle_mask, drift_gains, control_costs):
    planes, rows, cols, lanes = value_field.shape
    across, along = lax.axis_size("gx"), lax.axis_size("gy")
    sizes = dict(
        planes=planes, rows=rows, groups=cols // 2, width=lanes // QUARTERS,
        tiles=lanes // QUARTERS // LANES, row_total=rows * across, col_total=cols * along,
    )
    groups, width = sizes["groups"], sizes["width"]
    cells = planes * rows * cols * lanes
    full = (rows, groups, planes, 8, width)
    row_piece = (HALO, groups, planes, 8, width)
    col_piece = (rows, HALO, planes // 2, 8, width)
    pieces = [row_piece, row_piece, col_piece, col_piece]
    here = jnp.stack([lax.axis_index("gx"), lax.axis_index("gy")]).astype(jnp.int32)
    row_table, col_table = angle_tables(sizes)
    row_table, col_table, lane_table = jnp.asarray(row_table), jnp.asarray(col_table), jnp.asarray(lane_tables(sizes))
    value = to_blocks(value_field, sizes)
    ceiling = to_blocks(jnp.where(target_mask == 1, -0.5, BIG).astype(jnp.float32), sizes)
    floor = to_blocks(jnp.where(obstacle_mask == 1, 0.5, -BIG).astype(jnp.float32), sizes)

    prepare = call(prepare_kernel, sizes, pieces, [VMEM], "prepare", 1000)
    local = call(
        local_kernel, sizes, [full, (3,) + full, (3, 8, LANES)],
        [SMEM] * 5 + [VMEM] * 2, "local", 300 * cells,
    )
    column = call(
        column_kernel, sizes, [full, full, (1, 8, LANES)],
        [SMEM] * 4 + [VMEM] * 4, "column", 100 * cells,
    )
    row = call(
        row_kernel, sizes, [full, full, (across * along, 8, LANES)],
        [SMEM] * 2 + [VMEM] * 6, "row", 100 * cells,
    )
    update = call(
        update_kernel, sizes, [full] + pieces + [(8, LANES)], [VMEM] * 10, "update", 20 * cells
    )
    finish = call(update_kernel, sizes, [full, (8, LANES)], [VMEM] * 10, "finish", 20 * cells)

    first_rows, last_rows, first_cols, last_cols = prepare(value)
    up_x = [(i, (i + 1) % across) for i in range(across)]
    up_y = [(i, (i + 1) % along) for i in range(along)]
    down_x = [(j, i) for i, j in up_x]
    down_y = [(j, i) for i, j in up_y]
    step_sizes = []
    for number in range(STEPS):
        before = lax.ppermute(last_rows, "gx", up_x)
        after = lax.ppermute(first_rows, "gx", down_x)
        left = lax.ppermute(last_cols, "gy", up_y)
        right = lax.ppermute(first_cols, "gy", down_y)
        flow_local, jump_local, peak_local = local(
            here, drift_gains, control_costs, row_table, col_table, lane_table, value
        )
        flow_col, jump_col, peak_col = column(
            here, drift_gains, control_costs, row_table, lane_table, value, left, right
        )
        flow_row, jump_row, spread = row(
            drift_gains, control_costs, lane_table, value, before, after, peak_local, peak_col
        )
        gathered = lax.all_to_all(spread, ("gx", "gy"), 0, 0)
        operands = (value, ceiling, floor, flow_local, flow_col, flow_row, jump_local, jump_col, jump_row, gathered)
        if number < STEPS - 1:
            value, first_rows, last_rows, first_cols, last_cols, step_tile = update(*operands)
        else:
            value, step_tile = finish(*operands)
        step_sizes.append(step_tile[0, 0])
    return (from_blocks(value, sizes), jnp.stack(step_sizes))


def solution(mesh):
    return jax.shard_map(
        body,
        mesh=mesh,
        in_specs=(
            P(None, "gx", "gy", None),
            P(None, "gx", "gy", None),
            P(None, "gx", "gy", None),
            P(),
            P(),
        ),
        out_specs=(P(None, "gx", "gy", None), P()),
        check_vma=False,
    )
```

```python
import math

import jax
import jax.numpy as jnp
import numpy as np
from jax import lax
from jax.experimental import pallas as pl
from jax.experimental.pallas import tpu as pltpu
from jax.sharding import PartitionSpec as P

N3 = 32
N4 = 48
GRID = 96
STEPS = 3


courant = 0.5
weno_eps = 1e-06
LANES = 128
QUARTERS = 4
HALO = 3


def sub(a, b):
    if b is None:
        return a
    return -b if a is None else a - b


def square_term(inner, outer):
    constant = 0.3 * weno_eps
    if inner is None and outer is None:
        return constant
    if outer is None:
        return inner * inner + constant
    scaled = outer * 0.55
    rest = scaled * scaled * (0.0975 / 0.3025) + constant
    lean = sub(inner, scaled)
    return lean * lean + rest


def middle_term(left, right):
    constant = 0.75 * weno_eps
    if left is None and right is None:
        return constant
    if left is None or right is None:
        own = right if left is None else left
        return own * own + constant
    slope = right - left
    return slope * slope + (left * 0.75 * right + constant)


def bend(e_left, e_mid, e_right):
    return sub(sub(e_right, e_mid), sub(e_mid, e_left)) if e_mid is not None else (
        e_left if e_right is None else (e_right if e_left is None else e_left + e_right)
    )


def interface(e_one, e_two, e_three, e_four, inverse, minus, plus):
    first = square_term(e_two, e_one)
    second = middle_term(e_two, e_three)
    third = square_term(e_three, e_four)
    weight_one = second * third
    weight_two = first * third
    weight_three = first * second
    weight_one = weight_one * weight_one
    weight_two = weight_two * weight_two * 37.5
    weight_three = weight_three * weight_three
    bend_low = bend(e_one, e_two, e_three)
    bend_high = bend(e_two, e_three, e_four)
    result = []
    common = weight_one + weight_two + weight_three
    if minus:
        top = weight_one * (bend_low * (inverse / 6.0)) if bend_low is not None else 0.0
        high = bend_high * (inverse / 12.0)
        lower = common + (weight_three + weight_three)
        result.append((top + weight_three * high * 3.0) / lower - high * 0.5)
    if plus:
        top = weight_three * (bend_high * (inverse / 6.0)) if bend_high is not None else 0.0
        low = bend_low * (inverse / 12.0)
        lower = common + (weight_one + weight_one)
        result.append((top + weight_one * low * 3.0) / lower - low * 0.5)
    return result


def central(d_before, d_after, e_before, e_after, inverse):
    total = d_after if d_before is None else (d_before if d_after is None else d_before + d_after)
    tilt = sub(e_after, e_before)
    return total * (0.5 * inverse) - tilt * (inverse / 12.0)


def line_slopes(differences, inverse, cells):
    bends = [
        None if differences[j] is None and differences[j + 1] is None
        else sub(differences[j + 1], differences[j])
        for j in range(len(differences) - 1)
    ]
    minus = []
    plus = []
    for face in range(cells + 1):
        window = bends[face : face + 4]
        values = interface(*window, inverse, face < cells, face > 0)
        if face < cells:
            minus.append(values[0])
        if face > 0:
            plus.append(values[-1])
    out = []
    for cell in range(cells):
        base = central(
            differences[cell + 2], differences[cell + 3], bends[cell + 1], bends[cell + 3], inverse
        )
        out.append((base + (plus[cell] - minus[cell]), plus[cell] + minus[cell]))
    return out


def flux(middle, jump, drift, kappa):
    tilt = drift - kappa * middle
    return middle * (drift + tilt), jnp.abs(tilt) + kappa * jnp.abs(jump)


def sublane_turn(value):
    return pltpu.roll(value, 4, 0)


def spacings(sizes):
    return [
        2.0 / GRID,
        2.0 * math.pi / sizes["row_total"],
        2.0 * math.pi / sizes["col_total"],
        2.0 / GRID,
        2.0 / GRID,
    ]


def lane_shift(tiles, count, turn):
    number = len(tiles)
    lane = lax.broadcasted_iota(jnp.int32, (8, LANES), 1)
    spun = [pltpu.roll(tile, (-count) % LANES, 1) for tile in tiles]
    out = []
    for index in range(number):
        if count > 0:
            other = index + 1
            inside = lane < LANES - count
        else:
            other = index - 1
            inside = lane >= -count
        if 0 <= other < number:
            out.append(jnp.where(inside, spun[index], spun[other]))
        elif turn:
            wrapped = pltpu.roll(spun[other % number], 7 if count > 0 else 1, 0)
            out.append(jnp.where(inside, spun[index], wrapped))
        else:
            out.append(spun[index])
    return out


def lane_axis(tiles, stride, inverse, position, extent, turn, gather):
    number = range(len(tiles))
    first = [position[t] == 0 for t in number]
    last = [position[t] == extent - 1 for t in number]
    near_last = [position[t] >= extent - 2 for t in number]
    ahead = lane_shift(tiles, stride, turn)
    steps = [jnp.where(last[t], 0.0, ahead[t] - tiles[t]) for t in number]
    before = lane_shift(steps, -stride, turn)
    if not turn:
        before = [jnp.where(first[0], 0.0, before[0])] + before[1:]
    bends = [steps[t] - before[t] for t in number]
    down = lane_shift(bends, -stride, turn)
    down = [jnp.where(first[t], 0.0, down[t]) for t in number]
    up = lane_shift(bends, stride, turn)
    up = [jnp.where(last[t], 0.0, up[t]) for t in number]
    far = lane_shift(bends, 2 * stride, turn)
    far = [jnp.where(near_last[t], 0.0, far[t]) for t in number]
    minus = []
    plus = []
    for t in number:
        low, high = interface(down[t], bends[t], up[t], far[t], inverse, True, True)
        minus.append(low)
        plus.append(high)
    minus = lane_shift(minus, -stride, turn)
    if gather:
        own = bends[-1]
        over = up[-1]
        for t in number[:-1]:
            own = jnp.where(first[t], bends[t], own)
            over = jnp.where(first[t], up[t], over)
        edge = interface(None, None, own, over, inverse, True, False)[0]
        minus = [jnp.where(first[t], edge, minus[t]) for t in number]
    else:
        edge = interface(None, None, bends[0], up[0], inverse, True, False)[0]
        minus = [jnp.where(first[0], edge, minus[0])] + minus[1:]
    out = []
    for t in number:
        base = central(before[t], steps[t], down[t], up[t], inverse)
        out.append((base + (plus[t] - minus[t]), plus[t] + minus[t]))
    return out


def angle_tables(sizes):
    a = np.arange(sizes["row_total"], dtype=np.float64) * (2.0 * math.pi / sizes["row_total"])
    b = np.arange(sizes["col_total"], dtype=np.float64) * (2.0 * math.pi / sizes["col_total"])
    return (
        np.stack([np.cos(a), np.sin(a)]).astype(np.float32),
        np.stack([np.cos(b), np.sin(b)]).astype(np.float32),
    )


def lane_tables(sizes):
    lane = np.arange(sizes["width"])
    quarter = np.arange(8) % QUARTERS
    third = quarter[:, None] * (sizes["width"] // N4) + lane[None, :] // N4
    fourth = np.broadcast_to(lane[None, :] % N4, third.shape)
    return np.stack([third, fourth]).astype(np.float32)


def plane_position(plane, planes):
    return float((plane - planes / 2 + 0.5) * (2.0 / GRID))


def position_of(index, extent):
    return (index - extent / 2 + 0.5) * (2.0 / GRID)


def column_vector(table, kind, base, group, half, width=LANES):
    sublane = lax.broadcasted_iota(jnp.int32, (8, width), 0)
    low = jnp.full((8, width), table[kind, base + group], jnp.float32)
    high = jnp.full((8, width), table[kind, base + group + half], jnp.float32)
    return jnp.where(sublane < QUARTERS, low, high)


def local_kernel(sizes, where_ref, gains, costs, rows_ref, cols_ref, lanes_ref, value, flow, jump, peak):
    planes, rows, groups, tiles = sizes["planes"], sizes["rows"], sizes["groups"], sizes["tiles"]
    spacing = spacings(sizes)
    inverse = [1.0 / h for h in spacing]
    kappa = [costs[i] * spacing[i] for i in range(5)]
    row_base = where_ref[0] * rows
    col_base = where_ref[1] * 2 * groups

    def body(step, peaks):
        row = step // groups
        group = step % groups
        cos_a = rows_ref[0, row_base + row]
        cos_b = column_vector(cols_ref, 0, col_base, group, groups)
        sin_b = column_vector(cols_ref, 1, col_base, group, groups)
        third = [lanes_ref[0, :, pl.ds(t * LANES, LANES)] for t in range(tiles)]
        fourth = [lanes_ref[1, :, pl.ds(t * LANES, LANES)] for t in range(tiles)]
        block = [
            [value[row, group, p, :, pl.ds(t * LANES, LANES)] for t in range(tiles)]
            for p in range(planes)
        ]
        peak_zero, peak_three, peak_four = peaks
        total = [[None] * tiles for _ in range(planes)]
        for t in range(tiles):
            steps = [block[p + 1][t] - block[p][t] for p in range(planes - 1)]
            slopes = line_slopes([None] * 3 + steps + [None] * 3, inverse[0], planes)
            drift = gains[0] * (cos_a - 0.5 * cos_b + position_of(third[t], N3))
            for p in range(planes):
                middle, half_jump = slopes[p]
                part, speed = flux(middle, half_jump, drift, kappa[0])
                peak_zero = jnp.maximum(peak_zero, speed)
                total[p][t] = part
                jump[0, row, group, p, :, pl.ds(t * LANES, LANES)] = half_jump
        for p in range(planes):
            slopes = lane_axis(block[p], N4, inverse[3], third, N3, True, False)
            drift = gains[3] * (sin_b - plane_position(p, planes))
            for t in range(tiles):
                middle, half_jump = slopes[t]
                part, speed = flux(middle, half_jump, drift, kappa[3])
                peak_three = jnp.maximum(peak_three, speed)
                total[p][t] = total[p][t] + part
                jump[1, row, group, p, :, pl.ds(t * LANES, LANES)] = half_jump
            slopes = lane_axis(block[p], 1, inverse[4], fourth, N4, False, True)
            for t in range(tiles):
                middle, half_jump = slopes[t]
                drift = gains[4] * (cos_a * sin_b - position_of(fourth[t], N4))
                part, speed = flux(middle, half_jump, drift, kappa[4])
                peak_four = jnp.maximum(peak_four, speed)
                jump[2, row, group, p, :, pl.ds(t * LANES, LANES)] = half_jump
                flow[row, group, p, :, pl.ds(t * LANES, LANES)] = total[p][t] + part
        return peak_zero, peak_three, peak_four

    zero = jnp.zeros((8, LANES), jnp.float32)
    peaks = lax.fori_loop(0, rows * groups, body, (zero, zero, zero))
    for i in range(3):
        peak[i] = peaks[i]


def column_kernel(sizes, where_ref, gains, costs, rows_ref, lanes_ref, value, near, far, flow_in, flow, jump, peak):
    planes, rows, groups, tiles = sizes["planes"], sizes["rows"], sizes["groups"], sizes["tiles"]
    spacing = spacings(sizes)[2]
    kappa = costs[2] * spacing
    row_base = where_ref[0] * rows
    lower = lax.broadcasted_iota(jnp.int32, (8, LANES), 0) < QUARTERS
    even = jnp.full((8, LANES), where_ref[1] % 2, jnp.int32) == 0

    def body(step, top):
        row = step // tiles
        lanes = pl.ds(pl.multiple_of((step % tiles) * LANES, LANES), LANES)
        third = lanes_ref[0, :, lanes]
        drift = gains[2] * (position_of(third, N3) + 0.5 * rows_ref[1, row_base + row])
        packs = []
        for p in range(planes // 2):
            one = [near[row, k, p, :, lanes] for k in range(HALO)]
            two = [far[row, k, p, :, lanes] for k in range(HALO)]
            packs.append((
                [jnp.where(even, two[k], one[k]) for k in range(HALO)],
                [jnp.where(even, one[k], two[k]) for k in range(HALO)],
            ))
        for p in range(planes):
            own = [value[row, g, p, :, lanes] for g in range(groups)]
            turned = [sublane_turn(own[g]) for g in range(groups)]
            packed_left, packed_right = packs[p % (planes // 2)]
            if p >= planes // 2:
                packed_left = [sublane_turn(x) for x in packed_left]
            else:
                packed_right = [sublane_turn(x) for x in packed_right]
            below = [jnp.where(lower, packed_left[k], turned[groups - HALO + k]) for k in range(HALO)]
            above = [jnp.where(lower, turned[k], packed_right[k]) for k in range(HALO)]
            line = below + own + above
            steps = [line[j + 1] - line[j] for j in range(len(line) - 1)]
            slopes = line_slopes(steps, 1.0 / spacing, groups)
            for g in range(groups):
                middle, half_jump = slopes[g]
                part, speed = flux(middle, half_jump, drift, kappa)
                top = jnp.maximum(top, speed)
                flow[row, g, p, :, lanes] = flow_in[row, g, p, :, lanes] + part
                jump[row, g, p, :, lanes] = half_jump
        return top

    peak[0] = lax.fori_loop(0, rows * tiles, body, jnp.zeros((8, LANES), jnp.float32))


def row_kernel(sizes, where_ref, gains, costs, lanes_ref, value, near, far, peak_local, peak_col, flow_in,
               jump_local, jump_col, flow, jump, spread, store, sems):
    planes, rows, groups, tiles = sizes["planes"], sizes["rows"], sizes["groups"], sizes["tiles"]
    spacing = spacings(sizes)[1]
    kappa = costs[1] * spacing
    even = jnp.full((8, LANES), where_ref[0] % 2, jnp.int32) == 0
    copies = [
        pltpu.make_async_copy(jump_local, store.at[pl.ds(0, 3)], sems.at[0]),
        pltpu.make_async_copy(jump_col, store.at[3], sems.at[1]),
    ]
    for copy in copies:
        copy.start()

    def body(step, top):
        group = step // tiles
        lanes = pl.ds(pl.multiple_of((step % tiles) * LANES, LANES), LANES)
        fourth = position_of(lanes_ref[1, :, lanes], N4)
        for p in range(planes):
            one = [near[k, group, p, :, lanes] for k in range(HALO)]
            two = [far[k, group, p, :, lanes] for k in range(HALO)]
            line = [jnp.where(even, two[k], one[k]) for k in range(HALO)]
            line += [value[r, group, p, :, lanes] for r in range(rows)]
            line += [jnp.where(even, one[k], two[k]) for k in range(HALO)]
            steps = [line[j + 1] - line[j] for j in range(len(line) - 1)]
            slopes = line_slopes(steps, 1.0 / spacing, rows)
            drift = gains[1] * (fourth - 0.3 * plane_position(p, planes))
            for r in range(rows):
                middle, half_jump = slopes[r]
                part, speed = flux(middle, half_jump, drift, kappa)
                top = jnp.maximum(top, speed)
                flow[r, group, p, :, lanes] = flow_in[r, group, p, :, lanes] + part
                jump[r, group, p, :, lanes] = half_jump
        return top

    top = lax.fori_loop(0, groups * tiles, body, jnp.zeros((8, LANES), jnp.float32))
    found = [peak_local[0], top, peak_col[0], peak_local[1], peak_local[2]]
    sublane = lax.broadcasted_iota(jnp.int32, (8, LANES), 0)
    packed = jnp.zeros((8, LANES), jnp.float32)
    for i in range(5):
        widest = jnp.max(found[i], axis=0, keepdims=True)
        packed = jnp.where(sublane == i, widest, packed)
    for device in range(spread.shape[0]):
        spread[device] = packed
    for copy in copies:
        copy.wait()


def update_kernel(sizes, last, *refs):
    planes, rows, groups, tiles = sizes["planes"], sizes["rows"], sizes["groups"], sizes["tiles"]
    spacing = spacings(sizes)
    if last:
        value, flow, jump_row, store, code, gathered, old_one, old_two = refs[:8]
        result, step_ref, store_buf, code_buf, store_sems, code_sems, out_buf, out_sems = refs[8:]
    else:
        where_ref, value, flow, jump_row, store, code, gathered = refs[:7]
        result, step_ref = refs[7:9]
        pieces = refs[9:13]
        store_buf, code_buf, store_sems, code_sems = refs[13:]
    fetches = []
    for r in range(rows):
        fetches.append((
            pltpu.make_async_copy(store.at[:, r], store_buf.at[:, r], store_sems.at[r]),
            pltpu.make_async_copy(code.at[r], code_buf.at[r], code_sems.at[r]),
        ))
        for copy in fetches[-1]:
            copy.start()
    best = gathered[0]
    for device in range(1, gathered.shape[0]):
        best = jnp.maximum(best, gathered[device])
    widest = jnp.max(best, axis=1, keepdims=True)
    bounds = [widest[i : i + 1, :] for i in range(5)]
    total = bounds[0] / spacing[0]
    for i in range(1, 5):
        total = total + bounds[i] / spacing[i]
    time_step = courant / (total + 1e-06)
    if last:
        step_ref[0] = old_one[0]
        step_ref[1] = old_two[0]
        step_ref[2] = time_step[0, 0]
    else:
        step_ref[0] = time_step[0, 0]
    half_step = jnp.broadcast_to(time_step * 0.5, (8, LANES))
    weights = [jnp.broadcast_to(time_step * bounds[i], (8, LANES)) for i in range(5)]

    puts = []
    for row in range(rows):
        for copy in fetches[row]:
            copy.wait()

        def body(step, carry, row=row):
            group = step // tiles
            tile = step % tiles
            lanes = pl.ds(pl.multiple_of(tile * LANES, LANES), LANES)
            for p in range(planes):
                at = (row, group, p, slice(None), lanes)
                moved = (
                    (weights[0] * store_buf[(0,) + at] + weights[3] * store_buf[(1,) + at])
                    + (weights[4] * store_buf[(2,) + at] + weights[2] * store_buf[(3,) + at])
                ) + (weights[1] * jump_row[at] - half_step * flow[at])
                new = value[at] + moved
                mark = code_buf[at]
                new = jnp.where(mark * mark == 1.0, jnp.minimum(new, -0.5), new)
                new = jnp.where(mark < 0.0, jnp.maximum(new, 0.5), new)
                if last:
                    for s in range(8):
                        place = pl.ds(pl.multiple_of((s % QUARTERS) * tiles * LANES + tile * LANES, LANES), LANES)
                        column = group + (s // QUARTERS) * groups
                        out_buf[row, column, pl.ds(p, 1), place] = new[s : s + 1]
                else:
                    result[at] = new
            return carry

        lax.fori_loop(0, groups * tiles, body, 0)
        if last:
            puts.append(pltpu.make_async_copy(out_buf.at[row], result.at[row], out_sems.at[row]))
            puts[-1].start()
    for copy in puts:
        copy.wait()
    if not last:
        send_pieces(sizes, where_ref, result, *pieces)


def send_pieces(sizes, where_ref, value, near_rows, far_rows, near_cols, far_cols):
    planes, rows, groups, tiles = sizes["planes"], sizes["rows"], sizes["groups"], sizes["tiles"]
    lower = lax.broadcasted_iota(jnp.int32, (8, LANES), 0) < QUARTERS
    half = planes // 2
    odd_row = where_ref[0] % 2
    even = jnp.full((8, LANES), where_ref[1] % 2, jnp.int32) == 0
    near_start = (rows - HALO) * (1 - odd_row)
    far_start = (rows - HALO) * odd_row
    for k in range(HALO):
        near_rows[k] = value[near_start + k]
        far_rows[k] = value[far_start + k]

    def body(row, carry):
        for k in range(HALO):
            for p in range(half):
                for t in range(tiles):
                    lanes = pl.ds(t * LANES, LANES)
                    one = value[row, k, p, :, lanes]
                    two = value[row, k, p + half, :, lanes]
                    first = jnp.where(lower, one, sublane_turn(two))
                    one = value[row, groups - HALO + k, p, :, lanes]
                    two = value[row, groups - HALO + k, p + half, :, lanes]
                    last = jnp.where(lower, sublane_turn(one), two)
                    near_cols[row, k, p, :, lanes] = jnp.where(even, last, first)
                    far_cols[row, k, p, :, lanes] = jnp.where(even, first, last)
        return carry

    lax.fori_loop(0, rows, body, 0)


def regroup(sizes, source, row, group, tile, plane):
    groups, tiles = sizes["groups"], sizes["tiles"]
    sublane = lax.broadcasted_iota(jnp.int32, (8, LANES), 0)
    out = None
    for s in range(8):
        place = pl.ds(pl.multiple_of((s % QUARTERS) * tiles * LANES + tile * LANES, LANES), LANES)
        piece = source[row, group + (s // QUARTERS) * groups, pl.ds(plane, 1), place]
        piece = jnp.broadcast_to(piece, (8, LANES))
        out = piece if out is None else jnp.where(sublane == s, piece, out)
    return out


def prepare_kernel(sizes, where_ref, source, value, *pieces):
    planes, rows, groups, tiles = sizes["planes"], sizes["rows"], sizes["groups"], sizes["tiles"]

    def body(step, carry):
        row = step // groups
        group = step % groups
        for t in range(tiles):
            for p in range(planes):
                value[row, group, p, :, pl.ds(t * LANES, LANES)] = regroup(sizes, source, row, group, t, p)
        return carry

    lax.fori_loop(0, rows * groups, body, 0)
    send_pieces(sizes, where_ref, value, *pieces)


def mask_kernel(sizes, target, obstacle, code, buffer, sem):
    planes, rows, groups, tiles = sizes["planes"], sizes["rows"], sizes["groups"], sizes["tiles"]

    def body(step, carry):
        row = step // groups
        group = step % groups
        for t in range(tiles):
            for p in range(planes):
                hit = (regroup(sizes, target, row, group, t, p) == 1).astype(jnp.float32)
                wall = (regroup(sizes, obstacle, row, group, t, p) == 1).astype(jnp.float32)
                buffer[row, group, p, :, pl.ds(t * LANES, LANES)] = hit - 2.0 * wall
        return carry

    lax.fori_loop(0, rows * groups, body, 0)
    copy = pltpu.make_async_copy(buffer, code, sem)
    copy.start()
    copy.wait()


VMEM = pl.BlockSpec(memory_space=pltpu.VMEM)
SMEM = pl.BlockSpec(memory_space=pltpu.SMEM)
HBM = pl.BlockSpec(memory_space=pltpu.HBM)


def call(kernel, sizes, outs, out_specs, specs, flops, scratch=()):
    return pl.pallas_call(
        lambda *refs: kernel(sizes, *refs),
        out_shape=[jax.ShapeDtypeStruct(shape, jnp.float32) for shape in outs],
        in_specs=specs,
        out_specs=out_specs,
        scratch_shapes=list(scratch),
        compiler_params=pltpu.CompilerParams(vmem_limit_bytes=8 * 1024 * 1024),
        cost_estimate=pl.CostEstimate(flops=flops, bytes_accessed=1000000, transcendentals=0),
    )


def pairs(devices, offset):
    first = [((2 * k + offset) % devices, (2 * k + 1 + offset) % devices) for k in range(devices // 2)]
    return first + [(j, i) for i, j in first]


def body(value_field, target_mask, obstacle_mask, drift_gains, control_costs):
    planes, rows, cols, lanes = value_field.shape
    across, along = lax.axis_size("gx"), lax.axis_size("gy")
    sizes = dict(
        planes=planes, rows=rows, groups=cols // 2, width=lanes // QUARTERS,
        tiles=lanes // QUARTERS // LANES, row_total=rows * across, col_total=cols * along,
    )
    groups, width = sizes["groups"], sizes["width"]
    cells = planes * rows * cols * lanes
    full = (rows, groups, planes, 8, width)
    row_piece = (HALO, groups, planes, 8, width)
    col_piece = (rows, HALO, planes // 2, 8, width)
    pieces = [row_piece, row_piece, col_piece, col_piece]
    spread_shape = (across * along, 8, LANES)
    here = jnp.stack([lax.axis_index("gx"), lax.axis_index("gy")]).astype(jnp.int32)
    row_table, col_table = angle_tables(sizes)
    row_table, col_table, lane_table = jnp.asarray(row_table), jnp.asarray(col_table), jnp.asarray(lane_tables(sizes))

    dma = pltpu.SemaphoreType.DMA
    fetch = [pltpu.VMEM((4,) + full, jnp.float32), pltpu.VMEM(full, jnp.float32), dma((rows,)), dma((rows,))]
    natural = (rows, cols, planes, lanes)
    prepare = call(prepare_kernel, sizes, [full] + pieces, [VMEM] * 5, [SMEM, VMEM], 20 * cells)
    encode = call(
        mask_kernel, sizes, [full], [HBM], [VMEM] * 2, 20 * cells,
        [pltpu.VMEM(full, jnp.float32), dma],
    )
    local = call(
        local_kernel, sizes, [full, (3,) + full, (3, 8, LANES)], [VMEM] * 3,
        [SMEM] * 5 + [VMEM] * 2, 300 * cells,
    )
    column = call(
        column_kernel, sizes, [full, full, (1, 8, LANES)], [VMEM] * 3,
        [SMEM] * 4 + [VMEM] * 5, 100 * cells,
    )
    row = call(
        row_kernel, sizes, [full, full, spread_shape, (4,) + full], [VMEM] * 3 + [HBM],
        [SMEM] * 3 + [VMEM] * 9, 100 * cells, [dma((2,))],
    )
    sources = [VMEM] * 3 + [HBM] * 2 + [VMEM]
    update = call(
        lambda sizes, *refs: update_kernel(sizes, False, *refs), sizes, [full, (1,)] + pieces,
        [VMEM, SMEM] + [VMEM] * 4, [SMEM] + sources, 20 * cells, fetch,
    )
    finish = call(
        lambda sizes, *refs: update_kernel(sizes, True, *refs), sizes, [natural, (STEPS,)],
        [HBM, SMEM], sources + [SMEM] * 2, 20 * cells,
        fetch + [pltpu.VMEM(natural, jnp.float32), dma((rows,))],
    )

    turn = lambda array: array.transpose(1, 2, 0, 3)
    value, near_rows, far_rows, near_cols, far_cols = prepare(here, turn(value_field))
    (code,) = encode(turn(target_mask), turn(obstacle_mask))
    step_sizes = []
    for number in range(STEPS):
        near_row = lax.ppermute(near_rows, "gx", pairs(across, 0))
        far_row = lax.ppermute(far_rows, "gx", pairs(across, 1))
        near_col = lax.ppermute(near_cols, "gy", pairs(along, 0))
        far_col = lax.ppermute(far_cols, "gy", pairs(along, 1))
        flow, jump_local, peak_local = local(here, drift_gains, control_costs, row_table, col_table, lane_table, value)
        flow, jump_col, peak_col = column(
            here, drift_gains, control_costs, row_table, lane_table, value, near_col, far_col, flow
        )
        flow, jump_row, spread, store = row(
            here, drift_gains, control_costs, lane_table, value, near_row, far_row, peak_local, peak_col,
            flow, jump_local, jump_col,
        )
        gathered = lax.all_to_all(spread, ("gx", "gy"), 0, 0)
        operands = (value, flow, jump_row, store, code, gathered)
        if number < STEPS - 1:
            value, step_size, near_rows, far_rows, near_cols, far_cols = update(here, *operands)
            step_sizes.append(step_size)
        else:
            value, all_steps = finish(*operands, *step_sizes)
    return (value.transpose(2, 0, 1, 3), all_steps)


def solution(mesh):
    return jax.shard_map(
        body,
        mesh=mesh,
        in_specs=(
            P(None, "gx", "gy", None),
            P(None, "gx", "gy", None),
            P(None, "gx", "gy", None),
            P(),
            P(),
        ),
        out_specs=(P(None, "gx", "gy", None), P()),
        check_vma=False,
    )
```
